128 devices in a mesh: dp: 8 (over z, core), mp: 16 (over y, x).
Axes of the slice: x: 4, y: 4, z: 4, core: 2. Of those that a mesh axis runs over, the one named last changes fastest.
Arguments:
- crop_hidden: bfloat16 [8, 1536, 8192], P(None, 'dp', 'mp'), may hold values from -15 to 15
- projector_weight: bfloat16 [8192, 8192], P('mp'), may hold values from -0.21213203 to 0.21213203
- pairing: int32 [8, 1536], P(None, 'dp'), may hold values from 0 to 191, as said below
Outputs:
- embeddings: float32 [8192, 8, 1536], P('mp', 'dp')
- loss_terms: float32 [4], replicated
The draws below stay inside these ranges and needn't reach their ends.
Inputs may be any that keep to these rules, and one draw needn't show every extreme that they name: Each aligned block of 192 entries of a row of pairing is a permutation of 0 to 191.
All inputs are finite; a program needn't handle non-finite values.
Results may differ from the reference program's by a relative error of at most 0.0003.
Values may be sent and summed in bfloat16 or wider, within the bound.
No kernel may reach another device: no remote copies, remote signals or barrier semaphores. Data moves between devices by JAX's collectives and lax.ppermute only.
A program may use at most 128 MiB of HBM per device.

```python
import math
import jax
import jax.numpy as jnp
from jax import lax

P_SIZE = 8192
CROPS = 8
B_DEV = 192
BATCH = 1536


def latent_field(latent_key, basis_key, exponent):
    latent_width = 512
    ranks = jnp.arange(1, latent_width + 1, dtype=jnp.float32)
    spectrum = ranks ** (-exponent)
    spectrum = spectrum / jnp.sum(spectrum)
    latent = jax.random.normal(latent_key, (CROPS * BATCH, latent_width), jnp.float32) * jnp.sqrt(spectrum)[None, :]
    basis = jnp.clip(jax.random.normal(basis_key, (latent_width, P_SIZE), jnp.float32), -6.0, 6.0)
    mixed = jnp.dot(latent, basis, precision=jax.lax.Precision.HIGHEST)
    return mixed.reshape(CROPS, BATCH, P_SIZE)


def draw_crop_hidden(key, part):
    noise_key = jax.random.fold_in(key, 0)
    scale_key = jax.random.fold_in(key, 1)
    latent_key = jax.random.fold_in(key, 3)
    basis_key = jax.random.fold_in(key, 4)
    row_scale = jnp.exp(jax.random.uniform(scale_key, (CROPS, BATCH, 1), jnp.float32, math.log(0.4), math.log(2.5)))
    noise = jnp.clip(jax.random.normal(noise_key, (CROPS, BATCH, P_SIZE), jnp.float32), -6.0, 6.0)
    correlated = latent_field(latent_key, basis_key, 0.7)
    values = 0.837 * correlated + 0.548 * noise
    values = jnp.clip(values, -6.0, 6.0)
    return (values * row_scale).astype(jnp.bfloat16)


def draw_projector_weight(key, part):
    noise_key, column_key = jax.random.split(key, 2)
    column_scale = jnp.exp(jax.random.uniform(column_key, (1, P_SIZE), jnp.float32, math.log(0.1), math.log(1.6)))
    values = jnp.clip(jax.random.normal(noise_key, (P_SIZE, P_SIZE), jnp.float32), -6.0, 6.0) * column_scale / P_SIZE ** 0.5
    return values.astype(jnp.bfloat16)


def draw_pairing(key, part):
    block_keys = jax.random.split(key, CROPS * (BATCH // B_DEV))
    shuffled = jax.vmap(lambda one_key: jax.random.permutation(one_key, B_DEV))(block_keys)
    return shuffled.reshape(CROPS, BATCH).astype(jnp.int32)


def setup_inputs(seed: int = 0) -> dict:
    splits = jax.random.split(jax.random.key(seed), 4)
    crop_hidden = draw_crop_hidden(jax.random.fold_in(splits[3], 71), 0)
    projector_weight = draw_projector_weight(jax.random.fold_in(splits[3], 71), 0)
    pairing = draw_pairing(jax.random.fold_in(splits[3], 71), 0)
    return dict(crop_hidden=crop_hidden, projector_weight=projector_weight, pairing=pairing)


def reference(crop_hidden, projector_weight, pairing):
    flat_rows = crop_hidden.reshape(CROPS * BATCH, P_SIZE)
    embedded = jnp.dot(flat_rows, projector_weight, preferred_element_type=jnp.float32)
    embeddings = jnp.transpose(embedded.reshape(CROPS, BATCH, P_SIZE), (2, 0, 1))
    block_start = jnp.arange(BATCH, dtype=jnp.int32) // B_DEV * B_DEV
    aligned_list = []
    for crop_index in range(CROPS):
        image_index = (block_start + pairing[crop_index]).astype(jnp.int32)
        image_order = jnp.argsort(image_index).astype(jnp.int32)
        aligned_list.append(jnp.take(embeddings[:, crop_index, :], image_order, axis=1))
    aligned = jnp.stack(aligned_list, axis=1)
    invariance = 0.0
    for anchor in range(2):
        differ = aligned - aligned[:, anchor:anchor + 1, :]
        invariance = invariance + jnp.sum(differ * differ)
    invariance_loss = invariance / (2 * (CROPS - 1) * BATCH * P_SIZE)
    hinge_total = 0.0
    off_total = 0.0
    for crop_index in range(CROPS):
        values = embeddings[:, crop_index, :]
        centered = values - lax.optimization_barrier(jnp.mean(values, axis=1, keepdims=True))
        variance = lax.optimization_barrier(jnp.sum(centered * centered, axis=1)) / (BATCH - 1)
        hinge_total = hinge_total + jnp.sum(jax.nn.relu(1.0 - jnp.sqrt(variance + 0.0001)))
        gram_block = jnp.dot(centered.T, centered, precision=lax.Precision.HIGHEST)
        off_total = off_total + jnp.sum(gram_block * gram_block) / ((BATCH - 1) * (BATCH - 1)) - jnp.sum(variance * variance)
    variance_loss = hinge_total / (CROPS * P_SIZE)
    covariance_loss = off_total / (CROPS * P_SIZE)
    total_loss = 25.0 * invariance_loss + 25.0 * variance_loss + covariance_loss
    loss_terms = jnp.stack([invariance_loss, variance_loss, covariance_loss, total_loss]).astype(jnp.float32)
    return (embeddings, loss_terms)
```

```python
import jax
import jax.numpy as jnp
from jax import lax
from jax.experimental import pallas as pl
from jax.experimental.pallas import tpu as pltpu
from jax.sharding import Mesh
from jax.sharding import PartitionSpec as P

MP = ("mp_0", "mp_1")
DP = ("dp_0", "dp_1")
AXES = ("dp_0", "dp_1", "mp_0", "mp_1")


highest = lax.Precision.HIGHEST
epsilon = 0.0001
GRAM_BLOCK = 128
CHUNKS = ((1, 2), (3, 4), (5, 6), (7,), (0,))


def shift(x, axis, size, step):
    return lax.ppermute(x, axis, [(i, (i + step) % size) for i in range(size)])


def flip(x, axis, size, mask):
    return lax.ppermute(x, axis, [(i, i ^ mask) for i in range(size)])


def total(x):
    for axis in AXES:
        size = lax.axis_size(axis)
        if size == 2:
            x = x + flip(x, axis, 2, 1)
        else:
            x = (x + flip(x, axis, size, 1)) + (flip(x, axis, size, 2) + flip(x, axis, size, 3))
    return x


def gather_weight(projector_weight, dp_index, dp_count):
    width_part, features = projector_weight.shape
    rows = width_part // dp_count
    planes = lax.axis_size("dp_0")
    own = lax.dynamic_slice(projector_weight, (dp_index * rows, 0), (rows, features))
    own = lax.all_to_all(own, MP, split_axis=1, concat_axis=0, tiled=True)
    feature_part = own.shape[1]
    mp_count = own.shape[0] // rows
    own = own.reshape(mp_count, 1, rows, feature_part)
    plane = lax.axis_index("dp_0")
    core = lax.axis_index("dp_1")
    full = jnp.zeros((mp_count, dp_count, rows, feature_part), own.dtype)
    for step in range(planes):
        piece = own if step == 0 else shift(own, "dp_0", planes, step)
        source = (plane - step) % planes
        other = flip(piece, "dp_1", 2, 1)
        full = lax.dynamic_update_slice(full, piece, (0, source * 2 + core, 0, 0))
        full = lax.dynamic_update_slice(full, other, (0, source * 2 + 1 - core, 0, 0))
    return full.reshape(mp_count * width_part, feature_part)


def gram_body(*refs):
    parts, (blocks, variance, rows) = refs[:-3], refs[-3:]
    count = sum(part.shape[0] for part in parts)
    mean = sum(jnp.sum(part[...], axis=0, keepdims=True) for part in parts) / count
    square = jnp.zeros_like(mean)
    start = 0
    for part in parts:
        centered = part[...] - mean
        square = square + jnp.sum(centered * centered, axis=0, keepdims=True)
        rows[start : start + part.shape[0], :] = centered.astype(rows.dtype)
        start += part.shape[0]
    variance[...] = square / (count - 1)
    n = count // GRAM_BLOCK
    spot = n
    for i in range(n):
        strip = lax.dot_general(
            rows[i * GRAM_BLOCK : (i + 1) * GRAM_BLOCK, :],
            rows[i * GRAM_BLOCK :, :],
            (((1,), (1,)), ((), ())),
            preferred_element_type=jnp.float32,
        )
        for k in range(i, n):
            at = i if k == i else spot
            spot += k != i
            block = strip[:, (k - i) * GRAM_BLOCK : (k - i + 1) * GRAM_BLOCK]
            blocks[at * GRAM_BLOCK : (at + 1) * GRAM_BLOCK, :] = block.astype(blocks.dtype)
    left = blocks.shape[0] - spot * GRAM_BLOCK
    if left:
        blocks[spot * GRAM_BLOCK :, :] = jnp.zeros((left, GRAM_BLOCK), blocks.dtype)


def gram_blocks(parts, group):
    count = sum(part.shape[0] for part in parts)
    width = parts[0].shape[1]
    n = count // GRAM_BLOCK
    total_blocks = -(-(n * (n + 1) // 2) // group) * group
    return pl.pallas_call(
        gram_body,
        out_shape=(
            jax.ShapeDtypeStruct((total_blocks * GRAM_BLOCK, GRAM_BLOCK), jnp.bfloat16),
            jax.ShapeDtypeStruct((1, width), jnp.float32),
        ),
        scratch_shapes=[pltpu.VMEM((count, width), jnp.bfloat16)],
        name="gram",
    )(*parts)


def local(crop_hidden, projector_weight, pairing):
    crop_count, local_rows, width_part = crop_hidden.shape
    features = projector_weight.shape[1]
    dp_count = lax.axis_size(DP)
    dp_index = lax.axis_index(DP)
    batch_rows = local_rows * dp_count

    rolled = lax.dynamic_slice(
        jnp.concatenate([crop_hidden, crop_hidden], axis=0),
        (dp_index, 0, 0),
        (crop_count, local_rows, width_part),
    )
    gathered = []
    for chunk in CHUNKS:
        piece = rolled[chunk[0] : chunk[0] + len(chunk)].reshape(-1, width_part)
        gathered.append(lax.all_gather(piece, MP, axis=1, tiled=True))

    weight = gather_weight(projector_weight, dp_index, dp_count)
    feature_part = weight.shape[1]

    mine = [None] * crop_count
    received = [None] * crop_count
    owned = jnp.zeros((dp_count, local_rows, feature_part), jnp.float32)
    for chunk, full in zip(CHUNKS, gathered):
        block = jnp.dot(full, weight, preferred_element_type=jnp.float32)
        for n, step in enumerate(chunk):
            part = block[n * local_rows : (n + 1) * local_rows]
            mine[step] = part
            if step:
                part = lax.ppermute(part, DP, [(i, (i + step) % dp_count) for i in range(dp_count)])
            received[step] = part
            source = (dp_index - step) % dp_count
            owned = lax.dynamic_update_slice(owned, part[None], (source, 0, 0))

    blocks, variance = gram_blocks(received, lax.axis_size(MP))
    hinge_sum = jnp.sum(jax.nn.relu(1.0 - jnp.sqrt(variance + epsilon)))
    diagonal_sq = jnp.sum(variance * variance)
    gram_part = lax.psum_scatter(blocks, MP, scatter_dimension=0, tiled=True).astype(jnp.float32)
    row = lax.broadcasted_iota(jnp.int32, gram_part.shape, 0)
    row = row + lax.axis_index(MP) * gram_part.shape[0]
    frobenius = jnp.sum(gram_part * gram_part * jnp.where(row < batch_rows, 1.0, 2.0))
    frobenius = frobenius / ((batch_rows - 1) * (batch_rows - 1))

    by_crop = jnp.stack(mine, axis=0)
    rolled_pairing = lax.dynamic_slice(
        jnp.concatenate([pairing, pairing], axis=0), (dp_index, 0), pairing.shape
    )
    images = jnp.arange(local_rows, dtype=jnp.int32)
    onehot = (images[None, :, None] == rolled_pairing[:, None, :]).astype(jnp.float32)
    aligned = jnp.einsum("cir,crj->cij", onehot, by_crop, precision=highest)
    invariance = 0.0
    for anchor in range(2):
        base = lax.dynamic_slice_in_dim(aligned, (anchor - dp_index) % crop_count, 1, axis=0)
        differ = aligned - base
        invariance = invariance + jnp.sum(differ * differ)

    totals = total(jnp.stack([invariance, hinge_sum, frobenius - diagonal_sq]))
    invariance_loss = totals[0] / (2 * (crop_count - 1) * batch_rows * features)
    variance_loss = totals[1] / (crop_count * features)
    covariance_loss = totals[2] / (crop_count * features)
    total_loss = 25.0 * invariance_loss + 25.0 * variance_loss + covariance_loss
    loss_terms = jnp.stack([invariance_loss, variance_loss, covariance_loss, total_loss])
    return (owned.reshape(batch_rows, feature_part).T[:, None, :], loss_terms)


def solution(mesh):
    torus = Mesh(mesh.devices.reshape(4, 2, 4, 4), ("dp_0", "dp_1", "mp_0", "mp_1"))
    placed = (P(None, DP, MP), P(MP, None), P(None, DP))
    return jax.shard_map(
        local, mesh=torus, in_specs=placed, out_specs=(P(MP, DP, None), P()), check_vma=False
    )
```

```python
import jax
import jax.numpy as jnp
from jax import lax
from jax.experimental import pallas as pl
from jax.experimental.pallas import tpu as pltpu
from jax.sharding import Mesh
from jax.sharding import PartitionSpec as P

MP = ("mp_0", "mp_1")
DP = ("dp_0", "dp_1")
AXES = ("mp_0", "mp_1", "dp_0", "dp_1")
RING = 4


epsilon = 0.0001
GRAM_BLOCK = 128


def shift(x, axis, step):
    return lax.ppermute(x, axis, [(i, (i + step) % RING) for i in range(RING)])


def swap(x):
    return lax.ppermute(x, "dp_1", [(0, 1), (1, 0)])


def total(values):
    count = lax.axis_size(AXES)
    row = jnp.concatenate([values, jnp.zeros(128 - values.shape[0], values.dtype)])
    rows = jnp.broadcast_to(row[None, :], (count, 128))
    rows = lax.all_to_all(rows, AXES, split_axis=0, concat_axis=0, tiled=True)
    return jnp.sum(rows, axis=0)


def assemble_body(places, *refs):
    parts, out = refs[:-1], refs[-1]
    rows = parts[0].shape[1]
    for n, part in enumerate(parts):
        start = pl.multiple_of(places[n] * rows, rows)
        out[:, pl.ds(start, rows), :] = part[...]


def assemble(parts, places):
    count, rows, width = parts[0].shape
    vmem = pl.BlockSpec(memory_space=pltpu.VMEM)
    return pl.pallas_call(
        assemble_body,
        in_specs=[pl.BlockSpec(memory_space=pltpu.SMEM)] + [vmem] * len(parts),
        out_specs=vmem,
        out_shape=jax.ShapeDtypeStruct((count, rows * len(parts), width), parts[0].dtype),
        compiler_params=pltpu.CompilerParams(vmem_limit_bytes=24 << 20),
        name="assemble",
    )(places, *parts)


def start_weight(projector_weight, dp_index, dp_count):
    width_part, features = projector_weight.shape
    rows = width_part // dp_count
    mp_count = lax.axis_size(MP)
    own = lax.dynamic_slice(projector_weight, (dp_index * rows, 0), (rows, features))
    own = own.reshape(rows, mp_count, features // mp_count).transpose(1, 0, 2)
    return lax.all_to_all(own, MP, split_axis=0, concat_axis=0, tiled=True)


def gather_weight(own, plane, core):
    parts, places = [], []
    for step in range(RING):
        piece = own if step == 0 else shift(own, "dp_0", step)
        source = (plane - step) % RING * 2
        parts += [piece, swap(piece)]
        places += [source + core, source + 1 - core]
    return assemble(parts, jnp.stack(places).astype(jnp.int32))


def ring(parts, axis):
    low, high = parts
    left_low = shift(low, axis, 1)
    right_low = shift(low, axis, -1)
    right_high = shift(high, axis, -1)
    left_high = shift(high, axis, 1)
    far_low = shift(left_low, axis, 1)
    far_high = shift(right_high, axis, -1)
    return (low, high), (left_low, left_high), (right_low, right_high), (far_low, far_high)


OWN, LEFT, RIGHT, FAR = 0, -1, 1, 2


def plane_gather(parts, first_axis, second_axis):
    own, left, right, far = (jnp.concatenate(pair) for pair in ring(parts, first_axis))
    row = {OWN: own, LEFT: left, RIGHT: right, FAR: far}
    pieces = {(OWN, early): x for early, x in row.items()}
    for early in (OWN, LEFT, RIGHT, FAR):
        pieces[LEFT, early] = shift(row[early], second_axis, 1)
    for early in (OWN, RIGHT, FAR, LEFT):
        pieces[RIGHT, early] = shift(row[early], second_axis, -1)
    for late, early, step in ((LEFT, OWN, 1), (LEFT, LEFT, 1), (RIGHT, RIGHT, -1), (RIGHT, FAR, -1)):
        pieces[FAR, early] = shift(pieces[late, early], second_axis, step)
    return pieces


def block_table(keys, x_first):
    y = lax.axis_index("mp_0")
    x = lax.axis_index("mp_1")
    table = []
    for late, early in keys:
        dy, dx = (late, early) if x_first else (early, late)
        table.append((y + dy) % RING * RING + (x + dx) % RING)
    return jnp.stack(table).astype(jnp.int32)


def product(parts, weight, table, base, i, j, tall, wide):
    value = None if base is None else base[i : i + tall, j : j + wide]
    for spot, part in enumerate(parts):
        piece = jnp.dot(
            part[i : i + tall, :],
            weight[table[spot], :, j : j + wide],
            preferred_element_type=jnp.float32,
        )
        value = piece if value is None else value + piece
    return value


def matmul_body(n, has_base, table, *refs):
    parts, weight, out = refs[:n], refs[n], refs[-1]
    base = refs[n + 1] if has_base else None
    rows, width = out.shape
    tall, wide = rows // 2, width // 2
    for i in range(0, rows, tall):
        for j in range(0, width, wide):
            out[i : i + tall, j : j + wide] = product(parts, weight, table, base, i, j, tall, wide)


def matmul(parts, weight, table, base=None):
    rows, depth = parts[0].shape
    width = weight.shape[2]
    count = len(parts)
    operands = list(parts) + [weight] + ([] if base is None else [base])
    vmem = pl.BlockSpec(memory_space=pltpu.VMEM)
    return pl.pallas_call(
        lambda *refs: matmul_body(len(parts), base is not None, *refs),
        in_specs=[pl.BlockSpec(memory_space=pltpu.SMEM)] + [vmem] * len(operands),
        out_specs=vmem,
        out_shape=jax.ShapeDtypeStruct((rows, width), jnp.float32),
        cost_estimate=pl.CostEstimate(
            flops=2 * count * rows * depth * width,
            transcendentals=0,
            bytes_accessed=2 * count * depth * (rows + width) + 4 * rows * width,
        ),
        compiler_params=pltpu.CompilerParams(vmem_limit_bytes=24 << 20),
        name="embed",
    )(table, *operands)


ALL = (OWN, LEFT, RIGHT, FAR)
STEPS = (
    [(OWN, early) for early in ALL],
    [(late, early) for late in (LEFT, RIGHT) for early in ALL],
    [(FAR, OWN), (FAR, RIGHT)],
)
LAST = [(FAR, LEFT), (FAR, FAR)]


def embed(pieces, weight, x_first):
    value = None
    for keys in STEPS:
        value = matmul([pieces[key] for key in keys], weight, block_table(keys, x_first), value)
    return value


def finish_body(n, local_rows, *refs):
    tables, weight, bases = refs[:2], refs[2], refs[3:5]
    parts = refs[5 : 5 + n], refs[5 + n : 5 + 2 * n]
    owned, keep, send, by_y, by_x, variance, rows = refs[5 + 2 * n :]
    count, width = owned.shape
    mean = jnp.zeros((1, width), jnp.float32)
    tall, wide = bases[0].shape[0] // 2, width // 2
    for h in range(2):
        for i in range(0, 2 * tall, tall):
            for j in range(0, width, wide):
                value = product(parts[h], weight, tables[h], bases[h], i, j, tall, wide)
                owned[h * 2 * tall + i : h * 2 * tall + i + tall, j : j + wide] = value
    for start in range(0, count, local_rows):
        value = owned[start : start + local_rows, :]
        mean = mean + jnp.sum(value, axis=0, keepdims=True)
        at = start // local_rows
        back = (0, 3, 1, 2)[at // 2]
        out = send if at % 2 else keep
        out[back] = value.astype(out.dtype)
    mean = mean / count
    square = jnp.zeros_like(mean)
    for start in range(0, count, local_rows):
        centered = owned[start : start + local_rows, :] - mean
        square = square + jnp.sum(centered * centered, axis=0, keepdims=True)
        rows[start : start + local_rows, :] = centered.astype(rows.dtype)
    variance[...] = square / (count - 1)
    blocks = count // GRAM_BLOCK
    half = by_y.shape[2]
    per = 2 * half // GRAM_BLOCK

    def store(at, block):
        owner, first = at // per, at % per * GRAM_BLOCK
        y, x = owner // RING, owner % RING
        split = min(max(half - first, 0), GRAM_BLOCK)
        if split:
            by_y[y, x, first : first + split, :] = block[:split]
        if split < GRAM_BLOCK:
            low = first + split - half
            by_x[x, y, low : low + GRAM_BLOCK - split, :] = block[split:]

    spot = blocks
    strip_rows = 2 * GRAM_BLOCK
    for i in range(0, blocks, 2):
        strip = lax.dot_general(
            rows[i * GRAM_BLOCK : i * GRAM_BLOCK + strip_rows, :],
            rows[i * GRAM_BLOCK :, :],
            (((1,), (1,)), ((), ())),
            preferred_element_type=jnp.float32,
        ).astype(by_y.dtype)
        for r in range(2):
            for k in range(i + r, blocks):
                at = i + r if k == i + r else spot
                spot += k != i + r
                store(
                    at,
                    strip[
                        r * GRAM_BLOCK : (r + 1) * GRAM_BLOCK,
                        (k - i) * GRAM_BLOCK : (k - i + 1) * GRAM_BLOCK,
                    ],
                )
    while spot < per * RING * RING:
        store(spot, jnp.zeros((GRAM_BLOCK, GRAM_BLOCK), by_y.dtype))
        spot += 1


def finish(tops, weight, bases, local_rows):
    count = sum(base.shape[0] for base in bases)
    width = bases[0].shape[1]
    n = count // GRAM_BLOCK
    per = -(-(n * (n + 1) // 2) // (RING * RING))
    half = jax.ShapeDtypeStruct((RING, RING, per * GRAM_BLOCK // 2, GRAM_BLOCK), jnp.bfloat16)
    back = jax.ShapeDtypeStruct((RING, local_rows, width), jnp.bfloat16)
    tables = [block_table(LAST, x_first) for x_first in (True, False)]
    operands = [weight, *bases] + [pieces[key] for pieces in tops for key in LAST]
    smem = pl.BlockSpec(memory_space=pltpu.SMEM)
    vmem = pl.BlockSpec(memory_space=pltpu.VMEM)
    return pl.pallas_call(
        lambda *refs: finish_body(len(LAST), local_rows, *refs),
        in_specs=[smem] * 2 + [vmem] * len(operands),
        out_specs=[vmem] * 6,
        out_shape=(
            jax.ShapeDtypeStruct((count, width), jnp.float32),
            back,
            back,
            half,
            half,
            jax.ShapeDtypeStruct((1, width), jnp.float32),
        ),
        scratch_shapes=[pltpu.VMEM((count, width), jnp.bfloat16)],
        cost_estimate=pl.CostEstimate(
            flops=2 * count * count * width, transcendentals=0, bytes_accessed=8 * count * width
        ),
        compiler_params=pltpu.CompilerParams(vmem_limit_bytes=40 << 20),
        name="finish",
    )(*tables, *operands)


def scatter_sum(x, axis):
    at = lax.axis_index(axis)
    value = lax.dynamic_index_in_dim(x, at, 0, keepdims=False).astype(jnp.float32)
    for step in (1, 3, 2):
        piece = lax.dynamic_index_in_dim(x, (at + step) % RING, 0, keepdims=False)
        value = value + shift(piece, axis, step).astype(jnp.float32)
    return value


def exchange(keep, send):
    swapped = swap(send)
    pairs = [jnp.stack([keep[dz], swapped[dz]]) for dz in range(RING)]
    return [pairs[dz] if dz == 0 else shift(pairs[dz], "dp_0", dz) for dz in range(RING)]


def local(crop_hidden, projector_weight, pairing):
    crop_count, local_rows, width_part = crop_hidden.shape
    features = projector_weight.shape[1]
    dp_count = lax.axis_size(DP)
    dp_index = lax.axis_index(DP)
    plane = lax.axis_index("dp_0")
    core = lax.axis_index("dp_1")
    batch_rows = local_rows * dp_count

    def crop_of(dz, dc):
        return (plane + dz) % RING * 2 + (core ^ dc)

    order = [(dz, dc) for dz in range(RING) for dc in range(2)]
    picked = [
        jnp.stack(
            [lax.dynamic_index_in_dim(crop_hidden, crop_of(dz, dc), 0, keepdims=False) for dz in range(RING)]
        )
        for dc in range(2)
    ]
    hidden = exchange(*picked)
    hidden = [part.reshape(2 * local_rows, width_part) for part in hidden]
    weight = gather_weight(start_weight(projector_weight, dp_index, dp_count), plane, core)
    feature_part = weight.shape[2]
    tops = (
        plane_gather((hidden[0], hidden[1]), "mp_1", "mp_0"),
        plane_gather((hidden[3], hidden[2]), "mp_0", "mp_1"),
    )
    bases = [embed(pieces, weight, x_first) for pieces, x_first in zip(tops, (True, False))]
    sources = [(dz, dc) for dz in (0, 1, 3, 2) for dc in range(2)]
    owned_rows, keep, send, by_y, by_x, variance = finish(tops, weight, bases, local_rows)
    hinge_sum = jnp.sum(jax.nn.relu(1.0 - jnp.sqrt(variance + epsilon)))
    diagonal_sq = jnp.sum(variance * variance)
    by_y = scatter_sum(by_y, "mp_0").astype(jnp.bfloat16)
    by_x = scatter_sum(by_x, "mp_1").astype(jnp.bfloat16)
    by_y = scatter_sum(by_y, "mp_1")
    by_x = scatter_sum(by_x, "mp_0")
    half = by_y.shape[0]
    row = lax.broadcasted_iota(jnp.int32, by_y.shape, 0)
    row = row + lax.axis_index(MP) * (2 * half)
    frobenius = jnp.sum(by_y * by_y * jnp.where(row < batch_rows, 1.0, 2.0))
    frobenius += jnp.sum(by_x * by_x * jnp.where(row + half < batch_rows, 1.0, 2.0))
    frobenius = frobenius / ((batch_rows - 1) * (batch_rows - 1))

    split = owned_rows.reshape(dp_count, local_rows, feature_part)
    parts = {key: split[n] for n, key in enumerate(sources)}
    owned = jnp.zeros((dp_count, local_rows, feature_part), jnp.float32)
    for (dz, dc), part in parts.items():
        source = (plane - dz) % RING * 2 + (core ^ dc)
        owned = lax.dynamic_update_slice(owned, part[None], (source, 0, 0))
    owned = owned.reshape(batch_rows, feature_part).T[:, None, :]

    back = exchange(keep, send)
    by_crop = jnp.concatenate([back[(-dz) % RING] for dz in range(RING)], axis=0)
    turned = jnp.concatenate(
        [lax.dynamic_index_in_dim(pairing, crop_of(*key), 0, keepdims=True) for key in order], axis=0
    )
    images = jnp.arange(local_rows, dtype=jnp.int32)
    onehot = (images[None, :, None] == turned[:, None, :]).astype(jnp.bfloat16)
    aligned = jnp.einsum("cir,crj->cij", onehot, by_crop, preferred_element_type=jnp.float32)
    invariance = 0.0
    for anchor in range(2):
        at = (0 - plane) % RING * 2 + (core ^ anchor)
        differ = aligned - lax.dynamic_slice_in_dim(aligned, at, 1, axis=0)
        invariance = invariance + jnp.sum(differ * differ)

    totals = total(jnp.stack([invariance, hinge_sum, frobenius - diagonal_sq]))
    invariance_loss = totals[0] / (2 * (crop_count - 1) * batch_rows * features)
    variance_loss = totals[1] / (crop_count * features)
    covariance_loss = totals[2] / (crop_count * features)
    total_loss = 25.0 * invariance_loss + 25.0 * variance_loss + covariance_loss
    loss_terms = jnp.stack([invariance_loss, variance_loss, covariance_loss, total_loss])
    return (owned, loss_terms)


def solution(mesh):
    torus = Mesh(mesh.devices.reshape(4, 2, 4, 4), ("dp_0", "dp_1", "mp_0", "mp_1"))
    placed = (P(None, DP, MP), P(MP, None), P(None, DP))
    return jax.shard_map(
        local, mesh=torus, in_specs=placed, out_specs=(P(MP, DP, None), P()), check_vma=False
    )
```

```python
import jax
import jax.numpy as jnp
from jax import lax
from jax.experimental import pallas as pl
from jax.experimental.pallas import tpu as pltpu
from jax.sharding import Mesh
from jax.sharding import PartitionSpec as P

MP = ("mp_0", "mp_1")
DP = ("dp_0", "dp_1")
AXES = ("mp_0", "mp_1", "dp_0", "dp_1")
RING = 4


epsilon = 0.0001
GRAM_BLOCK = 128


def shift(x, axis, step):
    return lax.ppermute(x, axis, [(i, (i + step) % RING) for i in range(RING)])


def swap(x):
    return lax.ppermute(x, "dp_1", [(0, 1), (1, 0)])


def assemble_body(places, *refs):
    parts, out = refs[:-1], refs[-1]
    rows = parts[0].shape[1]

    def step(i, carry):
        for n, part in enumerate(parts):
            start = pl.multiple_of(places[n] * rows, rows)
            out[i, pl.ds(start, rows), :] = part[i]
        return carry

    lax.fori_loop(0, out.shape[0], step, 0)


def assemble(parts, places):
    count, rows, width = parts[0].shape
    vmem = pl.BlockSpec(memory_space=pltpu.VMEM)
    return pl.pallas_call(
        assemble_body,
        in_specs=[pl.BlockSpec(memory_space=pltpu.SMEM)] + [vmem] * len(parts),
        out_specs=vmem,
        out_shape=jax.ShapeDtypeStruct((count, rows * len(parts), width), parts[0].dtype),
        compiler_params=pltpu.CompilerParams(vmem_limit_bytes=24 << 20),
        name="assemble",
    )(places, *parts)


def start_weight(projector_weight, dp_index, dp_count):
    width_part, features = projector_weight.shape
    rows = width_part // dp_count
    mp_count = lax.axis_size(MP)
    own = lax.dynamic_slice(projector_weight, (dp_index * rows, 0), (rows, features))
    own = own.reshape(rows, mp_count, features // mp_count).transpose(1, 0, 2)
    return lax.all_to_all(own, MP, split_axis=0, concat_axis=0, tiled=True)


def gather_weight(own, plane, core):
    parts, places = [], []
    for step in range(RING):
        piece = own if step == 0 else shift(own, "dp_0", step)
        source = (plane - step) % RING * 2
        parts += [piece, swap(piece)]
        places += [source + core, source + 1 - core]
    places = jnp.stack(places).astype(jnp.int32)
    return assemble(parts, places)


def ring(own, axis):
    half = own.shape[0] // 2
    left = shift(own, axis, 1)
    right = shift(own, axis, -1)
    low = shift(left[:half], axis, 1)
    high = shift(right[half:], axis, -1)
    return left, right, jnp.concatenate([low, high])


OWN, LEFT, RIGHT, FAR = 0, -1, 1, 2


def plane_gather(own, first_axis, second_axis):
    left, right, far = ring(own, first_axis)
    row = {OWN: own, LEFT: left, RIGHT: right, FAR: far}
    pieces = {(OWN, early): x for early, x in row.items()}
    for early in (OWN, LEFT, RIGHT, FAR):
        pieces[LEFT, early] = shift(row[early], second_axis, 1)
    for early in (OWN, RIGHT, LEFT, FAR):
        pieces[RIGHT, early] = shift(row[early], second_axis, -1)
    for late, early, step in ((LEFT, OWN, 1), (LEFT, LEFT, 1), (RIGHT, RIGHT, -1), (RIGHT, FAR, -1)):
        pieces[FAR, early] = shift(pieces[late, early], second_axis, step)
    return pieces


def block_table(keys, x_first):
    y = lax.axis_index("mp_0")
    x = lax.axis_index("mp_1")
    table = []
    for late, early in keys:
        dy, dx = (late, early) if x_first else (early, late)
        table.append((y + dy) % RING * RING + (x + dx) % RING)
    return jnp.stack(table).astype(jnp.int32)


def products(parts, weight, table, base, out, first, unroll=False):
    rows, width = base.shape if base is not None else out.shape
    tall, wide = rows // 2, width // 2

    def tile(t, carry):
        i = pl.multiple_of(t // 2 * tall, tall)
        j = pl.multiple_of(t % 2 * wide, wide)
        value = None if base is None else base[pl.ds(i, tall), pl.ds(j, wide)]
        for spot, part in enumerate(parts):
            piece = jnp.dot(
                part[pl.ds(i, tall), :],
                weight[table[spot], :, pl.ds(j, wide)],
                preferred_element_type=jnp.float32,
            )
            value = piece if value is None else value + piece
        out[pl.ds(pl.multiple_of(first + i, tall), tall), pl.ds(j, wide)] = value
        return carry

    lax.fori_loop(0, 4, tile, 0, unroll=unroll)


def matmul_body(n, has_base, table, *refs):
    products(refs[:n], refs[n], table, refs[n + 1] if has_base else None, refs[-1], 0)


def matmul(parts, weight, table, base=None):
    rows, depth = parts[0].shape
    width = weight.shape[2]
    count = len(parts)
    operands = list(parts) + [weight] + ([] if base is None else [base])
    vmem = pl.BlockSpec(memory_space=pltpu.VMEM)
    return pl.pallas_call(
        lambda *refs: matmul_body(len(parts), base is not None, *refs),
        in_specs=[pl.BlockSpec(memory_space=pltpu.SMEM)] + [vmem] * len(operands),
        out_specs=vmem,
        out_shape=jax.ShapeDtypeStruct((rows, width), jnp.float32),
        cost_estimate=pl.CostEstimate(
            flops=2 * count * rows * depth * width,
            transcendentals=0,
            bytes_accessed=2 * count * depth * (rows + width) + 4 * rows * width,
        ),
        compiler_params=pltpu.CompilerParams(vmem_limit_bytes=24 << 20),
        name="embed",
    )(table, *operands)


ALL = (OWN, LEFT, RIGHT, FAR)
STEPS = (
    [(OWN, early) for early in ALL],
    [(late, early) for late in (LEFT, RIGHT) for early in ALL],
    [(FAR, OWN), (FAR, RIGHT)],
)
LAST = [(FAR, LEFT), (FAR, FAR)]


def embed(pieces, weight, x_first):
    value = None
    for keys in STEPS:
        table = block_table(keys, x_first)
        value = matmul([pieces[key] for key in keys], weight, table, value)
    return value


def finish_body(n, local_rows, *refs):
    tables, places, weight, bases = refs[:2], refs[2], refs[3], refs[4:6]
    parts = refs[6 : 6 + n], refs[6 + n : 6 + 2 * n]
    owned, keep, send, by_y, by_x, variance, values, rows = refs[6 + 2 * n :]
    count, width = values.shape
    mean = jnp.zeros((1, width), jnp.float32)
    for h in range(2):
        products(parts[h], weight, tables[h], bases[h], values, h * (count // 2), True)
    for start in range(0, count, local_rows):
        value = values[start : start + local_rows, :]
        mean = mean + jnp.sum(value, axis=0, keepdims=True)
        at = start // local_rows
        owned[places[at]] = value
        back = (0, 3, 1, 2)[at // 2]
        out = send if at % 2 else keep
        out[back] = value.astype(out.dtype)
    mean = mean / count
    square = jnp.zeros_like(mean)
    for start in range(0, count, local_rows):
        centered = values[start : start + local_rows, :] - mean
        square = square + jnp.sum(centered * centered, axis=0, keepdims=True)
        rows[start : start + local_rows, :] = centered.astype(rows.dtype)
    variance[...] = square / (count - 1)
    blocks = count // GRAM_BLOCK
    half = by_y.shape[2]
    per = 2 * half // GRAM_BLOCK

    def store(at, block):
        owner, first = at // per, at % per * GRAM_BLOCK
        y, x = owner // RING, owner % RING
        split = min(max(half - first, 0), GRAM_BLOCK)
        if split:
            by_y[y, x, first : first + split, :] = block[:split]
        if split < GRAM_BLOCK:
            low = first + split - half
            by_x[x, y, low : low + GRAM_BLOCK - split, :] = block[split:]

    spot = blocks
    strip_rows = 2 * GRAM_BLOCK
    for i in range(0, blocks, 2):
        strip = lax.dot_general(
            rows[i * GRAM_BLOCK : i * GRAM_BLOCK + strip_rows, :],
            rows[i * GRAM_BLOCK :, :],
            (((1,), (1,)), ((), ())),
            preferred_element_type=jnp.float32,
        ).astype(by_y.dtype)
        for r in range(2):
            for k in range(i + r, blocks):
                at = i + r if k == i + r else spot
                spot += k != i + r
                store(
                    at,
                    strip[
                        r * GRAM_BLOCK : (r + 1) * GRAM_BLOCK,
                        (k - i) * GRAM_BLOCK : (k - i + 1) * GRAM_BLOCK,
                    ],
                )
    while spot < per * RING * RING:
        store(spot, jnp.zeros((GRAM_BLOCK, GRAM_BLOCK), by_y.dtype))
        spot += 1


def finish(tops, weight, bases, places):
    count = sum(base.shape[0] for base in bases)
    width = bases[0].shape[1]
    local_rows = count // places.shape[0]
    n = count // GRAM_BLOCK
    per = -(-(n * (n + 1) // 2) // (RING * RING))
    half = jax.ShapeDtypeStruct((RING, RING, per * GRAM_BLOCK // 2, GRAM_BLOCK), jnp.bfloat16)
    back = jax.ShapeDtypeStruct((RING, local_rows, width), jnp.bfloat16)
    tables = [block_table(LAST, x_first) for x_first in (True, False)]
    operands = [weight, *bases] + [pieces[key] for pieces in tops for key in LAST]
    smem = pl.BlockSpec(memory_space=pltpu.SMEM)
    vmem = pl.BlockSpec(memory_space=pltpu.VMEM)
    return pl.pallas_call(
        lambda *refs: finish_body(len(LAST), local_rows, *refs),
        in_specs=[smem] * 3 + [vmem] * len(operands),
        out_specs=[vmem] * 6,
        out_shape=(
            jax.ShapeDtypeStruct((count // local_rows, local_rows, width), jnp.float32),
            back,
            back,
            half,
            half,
            jax.ShapeDtypeStruct((1, width), jnp.float32),
        ),
        scratch_shapes=[
            pltpu.VMEM((count, width), jnp.float32),
            pltpu.VMEM((count, width), jnp.bfloat16),
        ],
        cost_estimate=pl.CostEstimate(
            flops=2 * count * count * width, transcendentals=0, bytes_accessed=8 * count * width
        ),
        compiler_params=pltpu.CompilerParams(vmem_limit_bytes=40 << 20),
        name="finish",
    )(*tables, places, *operands)


def scatter(x, axis):
    at = lax.axis_index(axis)
    blocks = [lax.dynamic_index_in_dim(x, at, 0, keepdims=False)]
    for step in (1, 3, 2):
        piece = lax.dynamic_index_in_dim(x, (at + step) % RING, 0, keepdims=False)
        blocks.append(shift(piece, axis, step))
    return blocks


def add(blocks):
    return sum(block.astype(jnp.float32) for block in blocks)


def score_body(place, invariance, variance, *refs):
    parts, out = refs[:-1], refs[-1]
    count = len(parts) // 2
    half = parts[0].shape[0]
    diagonal = place[1]
    value = jnp.zeros((8, GRAM_BLOCK), jnp.float32)
    for h in range(2):
        block = add([part[...] for part in parts[h * count : (h + 1) * count]])
        row = lax.broadcasted_iota(jnp.int32, block.shape, 0) + (2 * place[0] + h) * half
        block = block * block * jnp.where(row < diagonal, 1.0, 2.0)
        value = value + jnp.sum(block.reshape(half // 8, 8, GRAM_BLOCK), axis=0)
    frobenius = jnp.sum(value) / ((diagonal - 1) * (diagonal - 1)).astype(jnp.float32)
    spread = variance[...]
    hinge = jnp.sum(jnp.maximum(1.0 - jnp.sqrt(spread + epsilon), 0.0))
    off = frobenius - jnp.sum(spread * spread)
    lane = lax.broadcasted_iota(jnp.int32, out.shape, 1)
    row = jnp.where(lane == 0, invariance[0, 0], jnp.where(lane == 1, hinge, off))
    out[...] = jnp.where(lane < 3, row, 0.0)


def score(place, invariance, variance, by_y, by_x):
    smem = pl.BlockSpec(memory_space=pltpu.SMEM)
    vmem = pl.BlockSpec(memory_space=pltpu.VMEM)
    parts = by_y + by_x
    return pl.pallas_call(
        score_body,
        in_specs=[smem] * 2 + [vmem] * (1 + len(parts)),
        out_specs=vmem,
        out_shape=jax.ShapeDtypeStruct((lax.axis_size(AXES), 128), jnp.float32),
        compiler_params=pltpu.CompilerParams(vmem_limit_bytes=16 << 20),
        name="score",
    )(place, invariance, variance, *parts)


def terms_body(scales, rows, out):
    sums = jnp.sum(rows[...], axis=0, keepdims=True)
    lane = lax.broadcasted_iota(jnp.int32, sums.shape, 1)
    losses = [jnp.sum(jnp.where(lane == n, sums, 0.0)) * scales[n] for n in range(3)]
    for n in range(3):
        out[n] = losses[n]
    out[3] = 25.0 * losses[0] + 25.0 * losses[1] + losses[2]


def loss_terms(rows, scales):
    rows = lax.all_to_all(rows, AXES, split_axis=0, concat_axis=0, tiled=True)
    smem = pl.BlockSpec(memory_space=pltpu.SMEM)
    return pl.pallas_call(
        terms_body,
        in_specs=[smem, pl.BlockSpec(memory_space=pltpu.VMEM)],
        out_specs=smem,
        out_shape=jax.ShapeDtypeStruct((4,), jnp.float32),
        compiler_params=pltpu.CompilerParams(vmem_limit_bytes=4 << 20),
        name="terms",
    )(jnp.array(scales, jnp.float32), rows)


def distances_body(anchors, images, *refs):
    parts, out, aligned = refs[:-2], refs[-2], refs[-1]
    count, size, width = aligned.shape

    for n, part in enumerate(parts):
        for k in range(2):
            at = 2 * n + k
            wanted = lax.broadcasted_iota(jnp.int32, (size, size), 0)
            onehot = jnp.where(wanted == images[at : at + 1, :], 1.0, 0.0).astype(part.dtype)
            aligned[at] = jnp.dot(onehot, part[k], preferred_element_type=jnp.float32)

    def step(at, value):
        for anchor in range(2):
            differ = aligned[at] - aligned[anchors[anchor]]
            value = value + jnp.sum((differ * differ).reshape(size // 8, 8, width), axis=0)
        return value

    value = lax.fori_loop(0, count, step, jnp.zeros((8, width), jnp.float32))
    out[0, 0] = jnp.sum(value)


def distances(anchors, images, parts):
    count, size = images.shape
    width = parts[0].shape[2]
    smem = pl.BlockSpec(memory_space=pltpu.SMEM)
    vmem = pl.BlockSpec(memory_space=pltpu.VMEM)
    value = pl.pallas_call(
        distances_body,
        in_specs=[smem] + [vmem] * (1 + len(parts)),
        out_specs=smem,
        out_shape=jax.ShapeDtypeStruct((1, 1), jnp.float32),
        scratch_shapes=[pltpu.VMEM((count, size, width), jnp.float32)],
        cost_estimate=pl.CostEstimate(
            flops=2 * count * size * size * width,
            transcendentals=0,
            bytes_accessed=2 * count * size * width,
        ),
        compiler_params=pltpu.CompilerParams(vmem_limit_bytes=16 << 20),
        name="distances",
    )(anchors, images, *parts)
    return value


def exchange(keep, send):
    swapped = swap(send)
    pairs = [jnp.stack([keep[dz], swapped[dz]]) for dz in range(RING)]
    return [pairs[dz] if dz == 0 else shift(pairs[dz], "dp_0", dz) for dz in range(RING)]


def local(crop_hidden, projector_weight, pairing):
    crop_count, local_rows, width_part = crop_hidden.shape
    features = projector_weight.shape[1]
    dp_count = lax.axis_size(DP)
    dp_index = lax.axis_index(DP)
    plane = lax.axis_index("dp_0")
    core = lax.axis_index("dp_1")
    batch_rows = local_rows * dp_count

    def crop_of(dz, dc):
        return (plane + dz) % RING * 2 + (core ^ dc)

    picked = [
        jnp.stack(
            [lax.dynamic_index_in_dim(crop_hidden, crop_of(dz, dc), 0, keepdims=False) for dz in range(RING)]
        )
        for dc in range(2)
    ]
    hidden = exchange(*picked)
    hidden = [part.reshape(2 * local_rows, width_part) for part in hidden]
    weight = gather_weight(start_weight(projector_weight, dp_index, dp_count), plane, core)
    feature_part = weight.shape[2]
    tops = (
        plane_gather(jnp.concatenate(hidden[:2]), "mp_1", "mp_0"),
        plane_gather(jnp.concatenate([hidden[3], hidden[2]]), "mp_0", "mp_1"),
    )
    bases = [embed(pieces, weight, x_first) for pieces, x_first in zip(tops, (True, False))]
    sources = [(dz, dc) for dz in (0, 1, 3, 2) for dc in range(2)]
    places = jnp.stack([(plane - dz) % RING * 2 + (core ^ dc) for dz, dc in sources])
    owned, keep, send, by_y, by_x, variance = finish(tops, weight, bases, places.astype(jnp.int32))
    by_y = add(scatter(by_y, "mp_0")).astype(jnp.bfloat16)
    by_x = add(scatter(by_x, "mp_1")).astype(jnp.bfloat16)
    by_y = scatter(by_y, "mp_1")
    by_x = scatter(by_x, "mp_0")

    owned = owned.reshape(batch_rows, feature_part).T[:, None, :]

    back = exchange(keep, send)
    turned = jnp.concatenate(
        [
            lax.dynamic_index_in_dim(pairing, crop_of(-dz, dc), 0, keepdims=True)
            for dz in range(RING)
            for dc in range(2)
        ],
        axis=0,
    )
    anchors = jnp.stack([plane * 2 + (core ^ anchor) for anchor in range(2)]).astype(jnp.int32)
    invariance = distances(anchors, turned, back)

    place = jnp.stack([lax.axis_index(MP), jnp.int32(batch_rows)]).astype(jnp.int32)
    rows = score(place, invariance, variance, by_y, by_x)
    scales = (
        1.0 / (2 * (crop_count - 1) * batch_rows * features),
        1.0 / (crop_count * features),
        1.0 / (crop_count * features),
    )
    return (owned, loss_terms(rows, scales))


def solution(mesh):
    torus = Mesh(mesh.devices.reshape(4, 2, 4, 4), ("dp_0", "dp_1", "mp_0", "mp_1"))
    placed = (P(None, DP, MP), P(MP, None), P(None, DP))
    return jax.shard_map(
        local, mesh=torus, in_specs=placed, out_specs=(P(MP, DP, None), P()), check_vma=False
    )
```

```python
import jax
import jax.numpy as jnp
from jax import lax
from jax.experimental import pallas as pl
from jax.experimental.pallas import tpu as pltpu
from jax.sharding import Mesh
from jax.sharding import PartitionSpec as P

MP = ("mp_0", "mp_1")
DP = ("dp_0", "dp_1")
AXES = ("mp_0", "mp_1", "dp_0", "dp_1")
RING = 4


epsilon = 0.0001
GRAM_BLOCK = 128


def shift(x, axis, step):
    return lax.ppermute(x, axis, [(i, (i + step) % RING) for i in range(RING)])


def swap(x):
    return lax.ppermute(x, "dp_1", [(0, 1), (1, 0)])


def assemble_body(places, *refs):
    parts, out = refs[:-1], refs[-1]
    rows = parts[0].shape[1]

    def step(i, carry):
        for n, part in enumerate(parts):
            start = pl.multiple_of(places[n] * rows, rows)
            out[i, pl.ds(start, rows), :] = part[i]
        return carry

    lax.fori_loop(0, out.shape[0], step, 0)


def assemble(parts, places):
    count, rows, width = parts[0].shape
    vmem = pl.BlockSpec(memory_space=pltpu.VMEM)
    return pl.pallas_call(
        assemble_body,
        in_specs=[pl.BlockSpec(memory_space=pltpu.SMEM)] + [vmem] * len(parts),
        out_specs=vmem,
        out_shape=jax.ShapeDtypeStruct((count, rows * len(parts), width), parts[0].dtype),
        compiler_params=pltpu.CompilerParams(vmem_limit_bytes=20 << 20),
        name="assemble",
    )(places, *parts)


def start_weight(projector_weight, dp_index, dp_count):
    width_part, features = projector_weight.shape
    rows = width_part // dp_count
    mp_count = lax.axis_size(MP)
    own = lax.dynamic_slice(projector_weight, (dp_index * rows, 0), (rows, features))
    own = own.reshape(rows, mp_count, features // mp_count).transpose(1, 0, 2)
    return lax.all_to_all(own, MP, split_axis=0, concat_axis=0, tiled=True)


def gather_weight(own, plane, core):
    parts, places = [], []
    for step in range(RING):
        piece = own if step == 0 else shift(own, "dp_0", step)
        source = (plane - step) % RING * 2
        parts += [piece, swap(piece)]
        places += [source + core, source + 1 - core]
    places = jnp.stack(places).astype(jnp.int32)
    return assemble(parts, places)


def ring(own, axis):
    half = own.shape[0] // 2
    left = shift(own, axis, 1)
    right = shift(own, axis, -1)
    low = left[:half]
    high = right[half:]
    low = shift(low, axis, 1)
    high = shift(high, axis, -1)
    return left, right, jnp.concatenate([low, high])


OWN, LEFT, RIGHT, FAR = 0, -1, 1, 2


def plane_gather(own, first_axis, second_axis):
    left, right, far = ring(own, first_axis)
    row = {OWN: own, LEFT: left, RIGHT: right, FAR: far}
    pieces = {(OWN, early): x for early, x in row.items()}
    for early in (OWN, LEFT, RIGHT, FAR):
        pieces[LEFT, early] = shift(row[early], second_axis, 1)
    for early in (OWN, RIGHT, LEFT, FAR):
        pieces[RIGHT, early] = shift(row[early], second_axis, -1)
    for late, early, step in ((LEFT, OWN, 1), (LEFT, LEFT, 1), (RIGHT, RIGHT, -1), (RIGHT, FAR, -1)):
        pieces[FAR, early] = shift(pieces[late, early], second_axis, step)
    return pieces


def block_table(keys, x_first):
    y = lax.axis_index("mp_0")
    x = lax.axis_index("mp_1")
    table = []
    for late, early in keys:
        dy, dx = (late, early) if x_first else (early, late)
        table.append((y + dy) % RING * RING + (x + dx) % RING)
    return jnp.stack(table).astype(jnp.int32)


def products(parts, weight, table, base, out, first, unroll=False):
    rows, width = base.shape if base is not None else out.shape
    tall, wide = rows // 2, width // 2

    def tile(t, carry):
        i = pl.multiple_of(t // 2 * tall, tall)
        j = pl.multiple_of(t % 2 * wide, wide)
        value = None if base is None else base[pl.ds(i, tall), pl.ds(j, wide)]
        for spot, part in enumerate(parts):
            piece = jnp.dot(
                part[pl.ds(i, tall), :],
                weight[table[spot], :, pl.ds(j, wide)],
                preferred_element_type=jnp.float32,
            )
            value = piece if value is None else value + piece
        out[pl.ds(pl.multiple_of(first + i, tall), tall), pl.ds(j, wide)] = value
        return carry

    lax.fori_loop(0, 4, tile, 0, unroll=unroll)


def matmul_body(n, has_base, table, *refs):
    products(refs[:n], refs[n], table, refs[n + 1] if has_base else None, refs[-1], 0)


def matmul(parts, weight, table, base=None):
    rows, depth = parts[0].shape
    width = weight.shape[2]
    count = len(parts)
    operands = list(parts) + [weight] + ([] if base is None else [base])
    vmem = pl.BlockSpec(memory_space=pltpu.VMEM)
    return pl.pallas_call(
        lambda *refs: matmul_body(len(parts), base is not None, *refs),
        in_specs=[pl.BlockSpec(memory_space=pltpu.SMEM)] + [vmem] * len(operands),
        out_specs=vmem,
        out_shape=jax.ShapeDtypeStruct((rows, width), jnp.float32),
        cost_estimate=pl.CostEstimate(
            flops=2 * count * rows * depth * width,
            transcendentals=0,
            bytes_accessed=2 * count * depth * (rows + width) + 4 * rows * width,
        ),
        compiler_params=pltpu.CompilerParams(vmem_limit_bytes=20 << 20),
        name="embed",
    )(table, *operands)


ALL = (OWN, LEFT, RIGHT, FAR)
STEPS = (
    [(OWN, early) for early in ALL],
    [(late, early) for late in (LEFT, RIGHT) for early in ALL],
    [(FAR, OWN), (FAR, RIGHT)],
)
LAST = [(FAR, LEFT), (FAR, FAR)]


def embed(pieces, weight, x_first):
    value = None
    for keys in STEPS:
        table = block_table(keys, x_first)
        value = matmul([pieces[key] for key in keys], weight, table, value)
    return value


def finish_body(n, local_rows, *refs):
    tables, places, weight, bases = refs[:2], refs[2], refs[3], refs[4:6]
    parts = refs[6 : 6 + n], refs[6 + n : 6 + 2 * n]
    owned, keep, send, by_y, by_x, variance, values, rows = refs[6 + 2 * n :]
    count, width = values.shape
    mean = jnp.zeros((1, width), jnp.float32)
    for h in range(2):
        products(parts[h], weight, tables[h], bases[h], values, h * (count // 2), True)
    for start in range(0, count, local_rows):
        value = values[start : start + local_rows, :]
        mean = mean + jnp.sum(value, axis=0, keepdims=True)
        at = start // local_rows
        owned[places[at]] = value
        back = (0, 3, 1, 2)[at // 2]
        out = send if at % 2 else keep
        out[back] = value.astype(out.dtype)
    mean = mean / count
    square = jnp.zeros_like(mean)
    for start in range(0, count, local_rows):
        centered = values[start : start + local_rows, :] - mean
        square = square + jnp.sum(centered * centered, axis=0, keepdims=True)
        rows[start : start + local_rows, :] = centered.astype(rows.dtype)
    variance[...] = square / (count - 1)
    blocks = count // GRAM_BLOCK
    half = by_y.shape[2]
    per = 2 * half // GRAM_BLOCK

    def store(at, block):
        owner, first = at // per, at % per * GRAM_BLOCK
        y, x = owner // RING, owner % RING
        split = min(max(half - first, 0), GRAM_BLOCK)
        if split:
            by_y[y, x, first : first + split, :] = block[:split]
        if split < GRAM_BLOCK:
            low = first + split - half
            by_x[x, y, low : low + GRAM_BLOCK - split, :] = block[split:]

    spot = blocks
    strip_rows = 2 * GRAM_BLOCK
    for i in range(0, blocks, 2):
        strip = lax.dot_general(
            rows[i * GRAM_BLOCK : i * GRAM_BLOCK + strip_rows, :],
            rows[i * GRAM_BLOCK :, :],
            (((1,), (1,)), ((), ())),
            preferred_element_type=jnp.float32,
        ).astype(by_y.dtype)
        for r in range(2):
            for k in range(i + r, blocks):
                at = i + r if k == i + r else spot
                spot += k != i + r
                store(
                    at,
                    strip[
                        r * GRAM_BLOCK : (r + 1) * GRAM_BLOCK,
                        (k - i) * GRAM_BLOCK : (k - i + 1) * GRAM_BLOCK,
                    ],
                )
    while spot < per * RING * RING:
        store(spot, jnp.zeros((GRAM_BLOCK, GRAM_BLOCK), by_y.dtype))
        spot += 1


def finish(tops, weight, bases, places):
    count = sum(base.shape[0] for base in bases)
    width = bases[0].shape[1]
    local_rows = count // places.shape[0]
    n = count // GRAM_BLOCK
    per = -(-(n * (n + 1) // 2) // (RING * RING))
    half = jax.ShapeDtypeStruct((RING, RING, per * GRAM_BLOCK // 2, GRAM_BLOCK), jnp.bfloat16)
    back = jax.ShapeDtypeStruct((RING, local_rows, width), jnp.bfloat16)
    tables = [block_table(LAST, x_first) for x_first in (True, False)]
    operands = [weight, *bases] + [pieces[key] for pieces in tops for key in LAST]
    smem = pl.BlockSpec(memory_space=pltpu.SMEM)
    vmem = pl.BlockSpec(memory_space=pltpu.VMEM)
    return pl.pallas_call(
        lambda *refs: finish_body(len(LAST), local_rows, *refs),
        in_specs=[smem] * 3 + [vmem] * len(operands),
        out_specs=[vmem] * 6,
        out_shape=(
            jax.ShapeDtypeStruct((count // local_rows, local_rows, width), jnp.float32),
            back,
            back,
            half,
            half,
            jax.ShapeDtypeStruct((1, width), jnp.float32),
        ),
        scratch_shapes=[
            pltpu.VMEM((count, width), jnp.float32),
            pltpu.VMEM((count, width), jnp.bfloat16),
        ],
        cost_estimate=pl.CostEstimate(
            flops=2 * count * count * width, transcendentals=0, bytes_accessed=8 * count * width
        ),
        compiler_params=pltpu.CompilerParams(vmem_limit_bytes=20 << 20),
        name="finish",
    )(*tables, places, *operands)


def scatter(x, axis):
    at = lax.axis_index(axis)
    blocks = [lax.dynamic_index_in_dim(x, at, 0, keepdims=False)]
    for step in (1, 3, 2):
        piece = lax.dynamic_index_in_dim(x, (at + step) % RING, 0, keepdims=False)
        blocks.append(shift(piece, axis, step))
    return blocks


def add(blocks):
    return sum(block.astype(jnp.float32) for block in blocks)


def score_body(place, invariance, variance, *refs):
    parts, out = refs[:-1], refs[-1]
    count = len(parts) // 2
    half = parts[0].shape[0]
    diagonal = place[1]
    value = jnp.zeros((8, GRAM_BLOCK), jnp.float32)
    for h in range(2):
        block = add([part[...] for part in parts[h * count : (h + 1) * count]])
        row = lax.broadcasted_iota(jnp.int32, block.shape, 0) + (2 * place[0] + h) * half
        block = block * block * jnp.where(row < diagonal, 1.0, 2.0)
        value = value + jnp.sum(block.reshape(half // 8, 8, GRAM_BLOCK), axis=0)
    frobenius = jnp.sum(value) / ((diagonal - 1) * (diagonal - 1)).astype(jnp.float32)
    spread = variance[...]
    hinge = jnp.sum(jnp.maximum(1.0 - jnp.sqrt(spread + epsilon), 0.0))
    off = frobenius - jnp.sum(spread * spread)
    lane = lax.broadcasted_iota(jnp.int32, out.shape, 1)
    row = jnp.where(lane == 0, invariance[0, 0], jnp.where(lane == 1, hinge, off))
    out[...] = jnp.where(lane < 3, row, 0.0)


def score(place, invariance, variance, by_y, by_x):
    smem = pl.BlockSpec(memory_space=pltpu.SMEM)
    vmem = pl.BlockSpec(memory_space=pltpu.VMEM)
    parts = by_y + by_x
    return pl.pallas_call(
        score_body,
        in_specs=[smem] * 2 + [vmem] * (1 + len(parts)),
        out_specs=vmem,
        out_shape=jax.ShapeDtypeStruct((lax.axis_size(AXES), 128), jnp.float32),
        compiler_params=pltpu.CompilerParams(vmem_limit_bytes=16 << 20),
        name="score",
    )(place, invariance, variance, *parts)


def terms_body(scales, rows, out):
    sums = jnp.sum(rows[...], axis=0, keepdims=True)
    lane = lax.broadcasted_iota(jnp.int32, sums.shape, 1)
    losses = [jnp.sum(jnp.where(lane == n, sums, 0.0)) * scales[n] for n in range(3)]
    for n in range(3):
        out[n] = losses[n]
    out[3] = 25.0 * losses[0] + 25.0 * losses[1] + losses[2]


def loss_terms(rows, scales):
    rows = lax.all_to_all(rows, AXES, split_axis=0, concat_axis=0, tiled=True)
    smem = pl.BlockSpec(memory_space=pltpu.SMEM)
    return pl.pallas_call(
        terms_body,
        in_specs=[smem, pl.BlockSpec(memory_space=pltpu.VMEM)],
        out_specs=smem,
        out_shape=jax.ShapeDtypeStruct((4,), jnp.float32),
        compiler_params=pltpu.CompilerParams(vmem_limit_bytes=4 << 20),
        name="terms",
    )(jnp.array(scales, jnp.float32), rows)


def distances_body(anchors, images, *refs):
    parts, out, aligned = refs[:-2], refs[-2], refs[-1]
    count, size, width = aligned.shape

    for n, part in enumerate(parts):
        for k in range(2):
            at = 2 * n + k
            wanted = lax.broadcasted_iota(jnp.int32, (size, size), 0)
            onehot = jnp.where(wanted == images[at : at + 1, :], 1.0, 0.0).astype(part.dtype)
            aligned[at] = jnp.dot(onehot, part[k], preferred_element_type=jnp.float32)

    def step(at, value):
        for anchor in range(2):
            differ = aligned[at] - aligned[anchors[anchor]]
            value = value + jnp.sum((differ * differ).reshape(size // 8, 8, width), axis=0)
        return value

    value = lax.fori_loop(0, count, step, jnp.zeros((8, width), jnp.float32))
    out[0, 0] = jnp.sum(value)


def distances(anchors, images, parts):
    count, size = images.shape
    width = parts[0].shape[2]
    smem = pl.BlockSpec(memory_space=pltpu.SMEM)
    vmem = pl.BlockSpec(memory_space=pltpu.VMEM)
    value = pl.pallas_call(
        distances_body,
        in_specs=[smem] + [vmem] * (1 + len(parts)),
        out_specs=smem,
        out_shape=jax.ShapeDtypeStruct((1, 1), jnp.float32),
        scratch_shapes=[pltpu.VMEM((count, size, width), jnp.float32)],
        cost_estimate=pl.CostEstimate(
            flops=2 * count * size * size * width,
            transcendentals=0,
            bytes_accessed=2 * count * size * width,
        ),
        compiler_params=pltpu.CompilerParams(vmem_limit_bytes=16 << 20),
        name="distances",
    )(anchors, images, *parts)
    return value


def pack_body(keep, swapped, *outs):
    for n, out in enumerate(outs):
        out[0] = keep[n]
        out[1] = swapped[n]


def pack(keep, swapped):
    count, rows, width = keep.shape
    vmem = pl.BlockSpec(memory_space=pltpu.VMEM)
    return pl.pallas_call(
        pack_body,
        in_specs=[vmem] * 2,
        out_specs=[vmem] * count,
        out_shape=[jax.ShapeDtypeStruct((2, rows, width), keep.dtype)] * count,
        compiler_params=pltpu.CompilerParams(vmem_limit_bytes=8 << 20),
        name="pack",
    )(keep, swapped)


def exchange(keep, send):
    pairs = pack(keep, swap(send))
    return [pairs[0]] + [shift(pairs[dz], "dp_0", dz) for dz in (1, 2, 3)]


def local(crop_hidden, projector_weight, pairing):
    crop_count, local_rows, width_part = crop_hidden.shape
    features = projector_weight.shape[1]
    dp_count = lax.axis_size(DP)
    dp_index = lax.axis_index(DP)
    plane = lax.axis_index("dp_0")
    core = lax.axis_index("dp_1")
    batch_rows = local_rows * dp_count

    def crop_of(dz, dc):
        return (plane + dz) % RING * 2 + (core ^ dc)

    picked = [
        jnp.stack(
            [lax.dynamic_index_in_dim(crop_hidden, crop_of(dz, dc), 0, keepdims=False) for dz in range(RING)]
        )
        for dc in range(2)
    ]
    hidden = exchange(*picked)
    hidden = [part.reshape(2 * local_rows, width_part) for part in hidden]
    weight = gather_weight(start_weight(projector_weight, dp_index, dp_count), plane, core)
    feature_part = weight.shape[2]
    tops = (
        plane_gather(jnp.concatenate(hidden[:2]), "mp_1", "mp_0"),
        plane_gather(jnp.concatenate([hidden[3], hidden[2]]), "mp_0", "mp_1"),
    )
    bases = [embed(pieces, weight, x_first) for pieces, x_first in zip(tops, (True, False))]
    sources = [(dz, dc) for dz in (0, 1, 3, 2) for dc in range(2)]
    places = jnp.stack([(plane - dz) % RING * 2 + (core ^ dc) for dz, dc in sources])
    turned = jnp.concatenate(
        [
            lax.dynamic_index_in_dim(pairing, crop_of(-dz, dc), 0, keepdims=True)
            for dz in range(RING)
            for dc in range(2)
        ],
        axis=0,
    )
    anchors = jnp.stack([plane * 2 + (core ^ anchor) for anchor in range(2)]).astype(jnp.int32)
    place = jnp.stack([lax.axis_index(MP), jnp.int32(batch_rows)]).astype(jnp.int32)
    places, turned, anchors, place = lax.optimization_barrier(
        (places.astype(jnp.int32), turned, anchors, place)
    )
    owned, keep, send, by_y, by_x, variance = finish(tops, weight, bases, places)
    by_y = scatter(by_y, "mp_0")
    by_x = scatter(by_x, "mp_1")
    by_y = add(by_y).astype(jnp.bfloat16)
    by_x = add(by_x).astype(jnp.bfloat16)
    by_y = scatter(by_y, "mp_1")
    by_x = scatter(by_x, "mp_0")

    owned = owned.reshape(batch_rows, feature_part).T[:, None, :]

    back = exchange(keep, send)
    invariance = distances(anchors, turned, back)

    rows = score(place, invariance, variance, by_y, by_x)
    scales = (
        1.0 / (2 * (crop_count - 1) * batch_rows * features),
        1.0 / (crop_count * features),
        1.0 / (crop_count * features),
    )
    return (owned, loss_terms(rows, scales))


def solution(mesh):
    torus = Mesh(mesh.devices.reshape(4, 2, 4, 4), ("dp_0", "dp_1", "mp_0", "mp_1"))
    placed = (P(None, DP, MP), P(MP, None), P(None, DP))
    return jax.shard_map(
        local, mesh=torus, in_specs=placed, out_specs=(P(MP, DP, None), P()), check_vma=False
    )
```

```python
import jax
import jax.numpy as jnp
from jax import lax
from jax.experimental import pallas as pl
from jax.experimental.pallas import tpu as pltpu
from jax.sharding import Mesh
from jax.sharding import PartitionSpec as P

MP = ("mp_0", "mp_1")
DP = ("dp_0", "dp_1")
AXES = ("mp_0", "mp_1", "dp_0", "dp_1")
RING = 4


epsilon = 0.0001
GRAM_BLOCK = 128


def shift(x, axis, step):
    return lax.ppermute(x, axis, [(i, (i + step) % RING) for i in range(RING)])


def swap(x):
    return lax.ppermute(x, "dp_1", [(0, 1), (1, 0)])


def assemble_body(places, *refs):
    parts, out = refs[:-1], refs[-1]
    rows = parts[0].shape[1]

    def step(i, carry):
        for n, part in enumerate(parts):
            start = pl.multiple_of(places[n] * rows, rows)
            out[i, pl.ds(start, rows), :] = part[i]
        return carry

    lax.fori_loop(0, out.shape[0], step, 0)


def assemble(parts, places):
    count, rows, width = parts[0].shape
    vmem = pl.BlockSpec(memory_space=pltpu.VMEM)
    return pl.pallas_call(
        assemble_body,
        in_specs=[pl.BlockSpec(memory_space=pltpu.SMEM)] + [vmem] * len(parts),
        out_specs=vmem,
        out_shape=jax.ShapeDtypeStruct((count, rows * len(parts), width), parts[0].dtype),
        compiler_params=pltpu.CompilerParams(vmem_limit_bytes=20 << 20),
        name="assemble",
    )(places, *parts)


def start_weight(projector_weight, dp_index, dp_count):
    width_part, features = projector_weight.shape
    rows = width_part // dp_count
    mp_count = lax.axis_size(MP)
    own = lax.dynamic_slice(projector_weight, (dp_index * rows, 0), (rows, features))
    own = own.reshape(rows, mp_count, features // mp_count).transpose(1, 0, 2)
    return lax.all_to_all(own, MP, split_axis=0, concat_axis=0, tiled=True)


def gather_weight(own, plane, core):
    parts, places = [], []
    for step in range(RING):
        piece = own if step == 0 else shift(own, "dp_0", step)
        source = (plane - step) % RING * 2
        parts += [piece, swap(piece)]
        places += [source + core, source + 1 - core]
    places = jnp.stack(places).astype(jnp.int32)
    return assemble(parts, places)


def ring(own, axis):
    half = own.shape[0] // 2
    left = shift(own, axis, 1)
    right = shift(own, axis, -1)
    low = left[:half]
    high = right[half:]
    low = shift(low, axis, 1)
    high = shift(high, axis, -1)
    return left, right, jnp.concatenate([low, high])


OWN, LEFT, RIGHT, FAR = 0, -1, 1, 2


def split_gather(first, second, first_axis, second_axis):
    parts = {}
    for tag, x in (("0", first), ("1", second)):
        parts[tag] = [
            shift(x, first_axis, 1),
            shift(x, first_axis, -1),
            shift(x, second_axis, 1),
            shift(x, second_axis, -1),
        ]
    low = shift(parts["0"][0], first_axis, 1)
    high = shift(parts["1"][1], first_axis, -1)
    left, right, above, below = (jnp.concatenate(pair) for pair in zip(*parts.values()))
    own, far = jnp.concatenate([first, second]), jnp.concatenate([low, high])
    return spread(own, left, right, far, second_axis, (above, below))


def plane_gather(own, first_axis, second_axis):
    left, right, far = ring(own, first_axis)
    return spread(own, left, right, far, second_axis)


def spread(own, left, right, far, second_axis, moved=None):
    row = {OWN: own, LEFT: left, RIGHT: right, FAR: far}
    pieces = {(OWN, early): x for early, x in row.items()}
    if moved:
        pieces[LEFT, OWN], pieces[RIGHT, OWN] = moved
    for early in (OWN, LEFT, RIGHT, FAR):
        if (LEFT, early) not in pieces:
            pieces[LEFT, early] = shift(row[early], second_axis, 1)
    for early in (OWN, RIGHT, LEFT, FAR):
        if (RIGHT, early) not in pieces:
            pieces[RIGHT, early] = shift(row[early], second_axis, -1)
    for late, early, step in ((LEFT, OWN, 1), (LEFT, LEFT, 1), (RIGHT, RIGHT, -1), (RIGHT, FAR, -1)):
        pieces[FAR, early] = shift(pieces[late, early], second_axis, step)
    return pieces


def block_table(keys, x_first):
    y = lax.axis_index("mp_0")
    x = lax.axis_index("mp_1")
    table = []
    for late, early in keys:
        dy, dx = (late, early) if x_first else (early, late)
        table.append((y + dy) % RING * RING + (x + dx) % RING)
    return jnp.stack(table).astype(jnp.int32)


def products(parts, weight, table, base, out, first, unroll=False):
    rows, width = base.shape if base is not None else out.shape
    tall, wide = rows // 2, width // 2

    def tile(t, carry):
        i = pl.multiple_of(t // 2 * tall, tall)
        j = pl.multiple_of(t % 2 * wide, wide)
        value = None if base is None else base[pl.ds(i, tall), pl.ds(j, wide)]
        for spot, part in enumerate(parts):
            piece = jnp.dot(
                part[pl.ds(i, tall), :],
                weight[table[spot], :, pl.ds(j, wide)],
                preferred_element_type=jnp.float32,
            )
            value = piece if value is None else value + piece
        out[pl.ds(pl.multiple_of(first + i, tall), tall), pl.ds(j, wide)] = value
        return carry

    lax.fori_loop(0, 4, tile, 0, unroll=unroll)


def matmul_body(n, has_base, table, *refs):
    products(refs[:n], refs[n], table, refs[n + 1] if has_base else None, refs[-1], 0)


def matmul(parts, weight, table, base=None):
    rows, depth = parts[0].shape
    width = weight.shape[2]
    count = len(parts)
    operands = list(parts) + [weight] + ([] if base is None else [base])
    vmem = pl.BlockSpec(memory_space=pltpu.VMEM)
    return pl.pallas_call(
        lambda *refs: matmul_body(len(parts), base is not None, *refs),
        in_specs=[pl.BlockSpec(memory_space=pltpu.SMEM)] + [vmem] * len(operands),
        out_specs=vmem,
        out_shape=jax.ShapeDtypeStruct((rows, width), jnp.float32),
        cost_estimate=pl.CostEstimate(
            flops=2 * count * rows * depth * width,
            transcendentals=0,
            bytes_accessed=2 * count * depth * (rows + width) + 4 * rows * width,
        ),
        compiler_params=pltpu.CompilerParams(vmem_limit_bytes=20 << 20),
        name="embed",
    )(table, *operands)


ALL = (OWN, LEFT, RIGHT, FAR)
STEPS = (
    [(OWN, early) for early in ALL],
    [(late, early) for late in (LEFT, RIGHT) for early in ALL],
    [(FAR, OWN), (FAR, RIGHT)],
)
LAST = [(FAR, LEFT), (FAR, FAR)]


def embed(pieces, weight, x_first):
    value = None
    for keys in STEPS:
        table = block_table(keys, x_first)
        value = matmul([pieces[key] for key in keys], weight, table, value)
    return value


def finish_body(n, local_rows, *refs):
    tables, places, weight, bases = refs[:2], refs[2], refs[3], refs[4:6]
    parts = refs[6 : 6 + n], refs[6 + n : 6 + 2 * n]
    owned, keep, send, by_y, by_x, variance, values, rows = refs[6 + 2 * n :]
    count, width = values.shape
    mean = jnp.zeros((1, width), jnp.float32)
    for h in range(2):
        products(parts[h], weight, tables[h], bases[h], values, h * (count // 2))

    def take(k, total):
        back = lax.select(k == 0, 0, lax.select(k == 1, 3, k - 1))
        for c, out in enumerate((keep, send)):
            at = 2 * k + c
            value = values[pl.ds(pl.multiple_of(at * local_rows, local_rows), local_rows), :]
            owned[places[at]] = value
            out[back] = value.astype(out.dtype)
            total = total + jnp.sum(value, axis=0, keepdims=True)
        return total

    mean = lax.fori_loop(0, RING, take, mean) / count

    def center(at, square):
        span = pl.ds(pl.multiple_of(at * local_rows, local_rows), local_rows)
        centered = values[span, :] - mean
        rows[span, :] = centered.astype(rows.dtype)
        return square + jnp.sum(centered * centered, axis=0, keepdims=True)

    square = lax.fori_loop(0, count // local_rows, center, jnp.zeros_like(mean))
    variance[...] = square / (count - 1)
    blocks = count // GRAM_BLOCK
    half = by_y.shape[2]
    per = 2 * half // GRAM_BLOCK

    def store(at, block):
        owner, first = at // per, at % per * GRAM_BLOCK
        y, x = owner // RING, owner % RING
        split = min(max(half - first, 0), GRAM_BLOCK)
        if split:
            by_y[y, x, first : first + split, :] = block[:split]
        if split < GRAM_BLOCK:
            low = first + split - half
            by_x[x, y, low : low + GRAM_BLOCK - split, :] = block[split:]

    spot = blocks
    strip_rows = 2 * GRAM_BLOCK
    for i in range(0, blocks, 2):
        strip = lax.dot_general(
            rows[i * GRAM_BLOCK : i * GRAM_BLOCK + strip_rows, :],
            rows[i * GRAM_BLOCK :, :],
            (((1,), (1,)), ((), ())),
            preferred_element_type=jnp.float32,
        ).astype(by_y.dtype)
        for r in range(2):
            for k in range(i + r, blocks):
                at = i + r if k == i + r else spot
                spot += k != i + r
                store(
                    at,
                    strip[
                        r * GRAM_BLOCK : (r + 1) * GRAM_BLOCK,
                        (k - i) * GRAM_BLOCK : (k - i + 1) * GRAM_BLOCK,
                    ],
                )
    while spot < per * RING * RING:
        store(spot, jnp.zeros((GRAM_BLOCK, GRAM_BLOCK), by_y.dtype))
        spot += 1


def finish(tops, weight, bases, places):
    count = sum(base.shape[0] for base in bases)
    width = bases[0].shape[1]
    local_rows = count // places.shape[0]
    n = count // GRAM_BLOCK
    per = -(-(n * (n + 1) // 2) // (RING * RING))
    half = jax.ShapeDtypeStruct((RING, RING, per * GRAM_BLOCK // 2, GRAM_BLOCK), jnp.bfloat16)
    back = jax.ShapeDtypeStruct((RING, local_rows, width), jnp.bfloat16)
    tables = [block_table(LAST, x_first) for x_first in (True, False)]
    operands = [weight, *bases] + [pieces[key] for pieces in tops for key in LAST]
    smem = pl.BlockSpec(memory_space=pltpu.SMEM)
    vmem = pl.BlockSpec(memory_space=pltpu.VMEM)
    return pl.pallas_call(
        lambda *refs: finish_body(len(LAST), local_rows, *refs),
        in_specs=[smem] * 3 + [vmem] * len(operands),
        out_specs=[vmem] * 6,
        out_shape=(
            jax.ShapeDtypeStruct((count // local_rows, local_rows, width), jnp.float32),
            back,
            back,
            half,
            half,
            jax.ShapeDtypeStruct((1, width), jnp.float32),
        ),
        scratch_shapes=[
            pltpu.VMEM((count, width), jnp.float32),
            pltpu.VMEM((count, width), jnp.bfloat16),
        ],
        cost_estimate=pl.CostEstimate(
            flops=2 * count * count * width, transcendentals=0, bytes_accessed=8 * count * width
        ),
        compiler_params=pltpu.CompilerParams(vmem_limit_bytes=20 << 20),
        name="finish",
    )(*tables, places, *operands)


def scatter(x, axis):
    at = lax.axis_index(axis)
    blocks = [lax.dynamic_index_in_dim(x, at, 0, keepdims=False)]
    for step in (1, 3, 2):
        piece = lax.dynamic_index_in_dim(x, (at + step) % RING, 0, keepdims=False)
        blocks.append(shift(piece, axis, step))
    return blocks


def add(blocks):
    return sum(block.astype(jnp.float32) for block in blocks)


def score_body(place, invariance, variance, *refs):
    parts, out = refs[:-1], refs[-1]
    count = len(parts) // 2
    half = parts[0].shape[0]
    diagonal = place[1]
    value = jnp.zeros((8, GRAM_BLOCK), jnp.float32)
    for h in range(2):
        block = add([part[...] for part in parts[h * count : (h + 1) * count]])
        row = lax.broadcasted_iota(jnp.int32, block.shape, 0) + (2 * place[0] + h) * half
        block = block * block * jnp.where(row < diagonal, 1.0, 2.0)
        value = value + jnp.sum(block.reshape(half // 8, 8, GRAM_BLOCK), axis=0)
    frobenius = jnp.sum(value) / ((diagonal - 1) * (diagonal - 1)).astype(jnp.float32)
    spread = variance[...]
    hinge = jnp.sum(jnp.maximum(1.0 - jnp.sqrt(spread + epsilon), 0.0))
    off = frobenius - jnp.sum(spread * spread)
    lane = lax.broadcasted_iota(jnp.int32, out.shape, 1)
    row = jnp.where(lane == 0, invariance[0, 0], jnp.where(lane == 1, hinge, off))
    out[...] = jnp.where(lane < 3, row, 0.0)


def score(place, invariance, variance, by_y, by_x):
    smem = pl.BlockSpec(memory_space=pltpu.SMEM)
    vmem = pl.BlockSpec(memory_space=pltpu.VMEM)
    parts = by_y + by_x
    return pl.pallas_call(
        score_body,
        in_specs=[smem] * 2 + [vmem] * (1 + len(parts)),
        out_specs=vmem,
        out_shape=jax.ShapeDtypeStruct((lax.axis_size(AXES), 128), jnp.float32),
        compiler_params=pltpu.CompilerParams(vmem_limit_bytes=16 << 20),
        name="score",
    )(place, invariance, variance, *parts)


def terms_body(scales, rows, out):
    sums = jnp.sum(rows[...], axis=0, keepdims=True)
    lane = lax.broadcasted_iota(jnp.int32, sums.shape, 1)
    losses = [jnp.sum(jnp.where(lane == n, sums, 0.0)) * scales[n] for n in range(3)]
    for n in range(3):
        out[n] = losses[n]
    out[3] = 25.0 * losses[0] + 25.0 * losses[1] + losses[2]


def loss_terms(rows, scales):
    rows = lax.all_to_all(rows, AXES, split_axis=0, concat_axis=0, tiled=True)
    smem = pl.BlockSpec(memory_space=pltpu.SMEM)
    return pl.pallas_call(
        terms_body,
        in_specs=[smem, pl.BlockSpec(memory_space=pltpu.VMEM)],
        out_specs=smem,
        out_shape=jax.ShapeDtypeStruct((4,), jnp.float32),
        compiler_params=pltpu.CompilerParams(vmem_limit_bytes=4 << 20),
        name="terms",
    )(jnp.array(scales, jnp.float32), rows)


def distances_body(anchors, images, *refs):
    parts, out, aligned = refs[:-2], refs[-2], refs[-1]
    count, size, width = aligned.shape

    for n, part in enumerate(parts):
        for k in range(2):
            at = 2 * n + k
            wanted = lax.broadcasted_iota(jnp.int32, (size, size), 0)
            onehot = jnp.where(wanted == images[at : at + 1, :], 1.0, 0.0).astype(part.dtype)
            aligned[at] = jnp.dot(onehot, part[k], preferred_element_type=jnp.float32)

    def step(at, value):
        for anchor in range(2):
            differ = aligned[at] - aligned[anchors[anchor]]
            value = value + jnp.sum((differ * differ).reshape(size // 8, 8, width), axis=0)
        return value

    value = lax.fori_loop(0, count, step, jnp.zeros((8, width), jnp.float32))
    out[0, 0] = jnp.sum(value)


def distances(anchors, images, parts):
    count, size = images.shape
    width = parts[0].shape[2]
    smem = pl.BlockSpec(memory_space=pltpu.SMEM)
    vmem = pl.BlockSpec(memory_space=pltpu.VMEM)
    value = pl.pallas_call(
        distances_body,
        in_specs=[smem] + [vmem] * (1 + len(parts)),
        out_specs=smem,
        out_shape=jax.ShapeDtypeStruct((1, 1), jnp.float32),
        scratch_shapes=[pltpu.VMEM((count, size, width), jnp.float32)],
        cost_estimate=pl.CostEstimate(
            flops=2 * count * size * size * width,
            transcendentals=0,
            bytes_accessed=2 * count * size * width,
        ),
        compiler_params=pltpu.CompilerParams(vmem_limit_bytes=16 << 20),
        name="distances",
    )(anchors, images, *parts)
    return value


def pack_body(keep, swapped, *outs):
    for n, out in enumerate(outs):
        out[0] = keep[n]
        out[1] = swapped[n]


def pack(keep, swapped):
    count, rows, width = keep.shape
    vmem = pl.BlockSpec(memory_space=pltpu.VMEM)
    return pl.pallas_call(
        pack_body,
        in_specs=[vmem] * 2,
        out_specs=[vmem] * count,
        out_shape=[jax.ShapeDtypeStruct((2, rows, width), keep.dtype)] * count,
        compiler_params=pltpu.CompilerParams(vmem_limit_bytes=8 << 20),
        name="pack",
    )(keep, swapped)


def exchange(keep, send):
    pairs = pack(keep, swap(send))
    return [pairs[0]] + [shift(pairs[dz], "dp_0", dz) for dz in (1, 2, 3)]


def local(crop_hidden, projector_weight, pairing):
    crop_count, local_rows, width_part = crop_hidden.shape
    features = projector_weight.shape[1]
    dp_count = lax.axis_size(DP)
    dp_index = lax.axis_index(DP)
    plane = lax.axis_index("dp_0")
    core = lax.axis_index("dp_1")
    batch_rows = local_rows * dp_count

    def crop_of(dz, dc):
        return (plane + dz) % RING * 2 + (core ^ dc)

    picked = [
        jnp.stack(
            [lax.dynamic_index_in_dim(crop_hidden, crop_of(dz, dc), 0, keepdims=False) for dz in range(RING)]
        )
        for dc in range(2)
    ]
    hidden = exchange(*picked)
    hidden = [part.reshape(2 * local_rows, width_part) for part in hidden]
    weight = gather_weight(start_weight(projector_weight, dp_index, dp_count), plane, core)
    feature_part = weight.shape[2]
    tops = (
        split_gather(hidden[0], hidden[1], "mp_1", "mp_0"),
        plane_gather(jnp.concatenate([hidden[3], hidden[2]]), "mp_0", "mp_1"),
    )
    bases = [embed(pieces, weight, x_first) for pieces, x_first in zip(tops, (True, False))]
    sources = [(dz, dc) for dz in (0, 1, 3, 2) for dc in range(2)]
    places = jnp.stack([(plane - dz) % RING * 2 + (core ^ dc) for dz, dc in sources])
    turned = jnp.concatenate(
        [
            lax.dynamic_index_in_dim(pairing, crop_of(-dz, dc), 0, keepdims=True)
            for dz in range(RING)
            for dc in range(2)
        ],
        axis=0,
    )
    anchors = jnp.stack([plane * 2 + (core ^ anchor) for anchor in range(2)]).astype(jnp.int32)
    place = jnp.stack([lax.axis_index(MP), jnp.int32(batch_rows)]).astype(jnp.int32)
    places, turned, anchors, place = lax.optimization_barrier(
        (places.astype(jnp.int32), turned, anchors, place)
    )
    owned, keep, send, by_y, by_x, variance = finish(tops, weight, bases, places)
    by_y = scatter(by_y, "mp_0")
    by_x = scatter(by_x, "mp_1")
    by_y = add(by_y).astype(jnp.bfloat16)
    by_x = add(by_x).astype(jnp.bfloat16)
    by_y = scatter(by_y, "mp_1")
    by_x = scatter(by_x, "mp_0")

    owned = owned.reshape(batch_rows, feature_part).T[:, None, :]

    back = exchange(keep, send)
    invariance = distances(anchors, turned, back)

    rows = score(place, invariance, variance, by_y, by_x)
    scales = (
        1.0 / (2 * (crop_count - 1) * batch_rows * features),
        1.0 / (crop_count * features),
        1.0 / (crop_count * features),
    )
    return (owned, loss_terms(rows, scales))


def solution(mesh):
    torus = Mesh(mesh.devices.reshape(4, 2, 4, 4), ("dp_0", "dp_1", "mp_0", "mp_1"))
    placed = (P(None, DP, MP), P(MP, None), P(None, DP))
    return jax.shard_map(
        local, mesh=torus, in_specs=placed, out_specs=(P(MP, DP, None), P()), check_vma=False
    )
```
